128 devices in a mesh: gx: 16 (over y, z), gy: 8 (over x, core).
Axes of the slice: x: 4, y: 4, z: 4, core: 2. Of those that a mesh axis runs over, the one named last changes fastest.
Arguments:
- forces: float32 [3, 256, 256, 256], P(None, 'gx', 'gy'), may hold values from -8 to 8
- pressure_prev: float32 [256, 256, 256], P('gx', 'gy'), may hold values from -8 to 8
Outputs:
- pressure: float32 [256, 256, 256], P('gx', 'gy')
- residual: float32 [256, 256, 256], P('gx', 'gy')
The draws below stay inside these ranges and needn't reach their ends.
All inputs are finite; a program needn't handle non-finite values.
Results may differ from the reference program's by a relative error of at most 0.0003.
Values sent between devices are 32-bit elements; how exact they have to be, the bound alone decides.
A program may use at most 64 MiB of HBM per device.

```python
import jax
import jax.numpy as jnp
from jax import lax

NZ = 256
LEVELS = 5
SWEEPS = 2
COARSE_SWEEPS = 4
CYCLES = 2
NX = 256
NY = 256


def draw_pressure_prev(key, part):
    noise_key = jax.random.fold_in(key, 11)
    profile_key = jax.random.fold_in(key, 23)
    profile = 2.5 * jax.random.normal(profile_key, (NZ,), jnp.float32)
    noise = jax.random.normal(noise_key, (NX, NY, NZ), jnp.float32)
    return jnp.clip(noise + profile[None, None, :], -8.0, 8.0).astype(jnp.float32)


def block_scale(key, dims, shards, low, top_value):
    loudness, own = 1.0, jax.random.fold_in(key, 6)
    for dim, parts in shards:
        heights = jnp.exp(jax.random.uniform(jax.random.fold_in(own, dim), (parts,), jnp.float32, low / len(shards), top_value / len(shards)))
        loudness = loudness * jnp.repeat(heights, dims[dim] // parts).reshape([-1 if axis == dim else 1 for axis in range(len(dims))])
    return loudness


def normal_values(own_key, shape, spread, most, pieces=(), kind=jnp.bfloat16):
    gain = block_scale(own_key, shape, pieces, -0.22, 0.18) if pieces else 1.0
    drawn = jax.random.normal(own_key, shape, jnp.float32) * spread * gain
    return jnp.minimum(jnp.maximum(drawn, -most), most).astype(kind)


def setup_inputs(seed: int = 0) -> dict:
    splits = jax.random.split(jax.random.key(seed), 3)
    return {
        "forces": normal_values(splits[0], (3, NX, NY, NZ), 1.0, 8.0, ((1, 16), (2, 8)), jnp.float32),
        "pressure_prev": draw_pressure_prev(jax.random.fold_in(splits[2], 71), 0),
    }


OMEGA = 0.8

def vertical(values):
    padded = jnp.pad(values, ((0, 0), (0, 0), (1, 1)))
    return padded[:, :, 2:] + padded[:, :, :-2]

def operate_padded(padded, weight):
    center = padded[1:-1, 1:-1]
    beside = padded[2:, 1:-1] + padded[:-2, 1:-1] + padded[1:-1, 2:] + padded[1:-1, :-2]
    return weight * (4.0 * center - beside) + (2.0 * center - vertical(center))

def relax(padded, source, weight):
    center = padded[1:-1, 1:-1]
    return center + OMEGA * (source - operate_padded(padded, weight)) / (4.0 * weight + 2.0)

def wrapped(values):
    return jnp.pad(values, ((1, 1), (1, 1), (0, 0)), mode='wrap')

def restrict(residual_now):
    rows_x, rows_y, depth = residual_now.shape
    return 0.25 * residual_now.reshape(rows_x // 2, 2, rows_y // 2, 2, depth).sum(axis=(1, 3))

def prolong(correction):
    return jnp.repeat(jnp.repeat(correction, 2, axis=0), 2, axis=1)

def mean_mode(values, source):
    depth = source.shape[2]
    column = jnp.mean(source, axis=(0, 1))
    lower = jnp.concatenate([jnp.zeros((1,), source.dtype), -jnp.ones((depth - 1,), source.dtype)])
    upper = jnp.concatenate([-jnp.ones((depth - 1,), source.dtype), jnp.zeros((1,), source.dtype)])
    middle = 2.0 * jnp.ones((depth,), source.dtype)
    profile = lax.linalg.tridiagonal_solve(lower, middle, upper, column[:, None])[:, 0]
    return values + profile[None, None, :]

def whole_cycle(values, source, level_index):
    weight = 0.25 ** level_index
    if level_index == LEVELS - 1:
        values = mean_mode(values, source)
        for sweep_index in range(COARSE_SWEEPS):
            values = relax(wrapped(values), source, weight)
        return values
    for sweep_index in range(SWEEPS):
        values = relax(wrapped(values), source, weight)
    residual_now = source - operate_padded(wrapped(values), weight)
    coarse_source = restrict(residual_now)
    correction = whole_cycle(jnp.zeros_like(coarse_source), coarse_source, level_index + 1)
    values = values + prolong(correction)
    for sweep_index in range(SWEEPS):
        values = relax(wrapped(values), source, weight)
    return values

def reference(forces, pressure_prev):
    force_x, force_y, force_z = (forces[0], forces[1], forces[2])
    behind_x = jnp.roll(force_x, 1, axis=0)
    behind_y = jnp.roll(force_y, 1, axis=1)
    behind_z = jnp.pad(force_z[:, :, :-1], ((0, 0), (0, 0), (1, 0)))
    source = behind_x - force_x + (behind_y - force_y) + (behind_z - force_z)
    pressure = pressure_prev
    for cycle_index in range(CYCLES):
        pressure = whole_cycle(pressure, source, 0)
    residual = source - operate_padded(wrapped(pressure), 1.0)
    return (pressure, residual)
```

```python
import functools

import jax
import jax.numpy as jnp
import numpy as np
from jax import lax
from jax.experimental import pallas as pl
from jax.experimental.pallas import tpu as pltpu
from jax.sharding import PartitionSpec as P

MESH = pl.DeviceIdType.MESH
OMEGA = 0.8
LEVELS = 5
GX, GY = 16, 8
NDEV = GX * GY
BX, BY, NZ = 16, 32, 256
HIGHEST = lax.Precision.HIGHEST


def sine_matrix(weight=1.0):
    k = np.arange(1, NZ + 1, dtype=np.float64)
    return (weight * (np.sqrt(2.0 / (NZ + 1)) * np.sin(np.pi * np.outer(k, k) / (NZ + 1)))).astype(np.float32)


def spectrum():
    k = np.arange(1, NZ + 1, dtype=np.float64)
    return 4.0 * np.sin(0.5 * np.pi * k / (NZ + 1)) ** 2


def eigenvalues():
    rows = np.tile(spectrum().reshape(NDEV, 2), (1, 4))
    return np.broadcast_to(rows[:, :, None], (NDEV, 8, 128)).astype(np.float32)


def iota(axis):
    return lax.broadcasted_iota(jnp.int32, (8, 128), axis)


def exchange_blocks(vectors, axis, unit):
    size = 4 * unit
    place = iota(axis) // unit
    low, even = place < 2, lax.rem(place, 2) == 0
    a = list(vectors)
    for i in (0, 1):
        x, y = a[i], a[i + 2]
        a[i] = jnp.where(low, x, pltpu.roll(y, 2 * unit, axis))
        a[i + 2] = jnp.where(low, pltpu.roll(x, 2 * unit, axis), y)
    for i in (0, 2):
        x, y = a[i], a[i + 1]
        a[i] = jnp.where(even, x, pltpu.roll(y, unit, axis))
        a[i + 1] = jnp.where(even, pltpu.roll(x, size - unit, axis), y)
    return a


def remap(grid):
    cols = [exchange_blocks([grid[q][g] for q in range(4)], 0, 2) for g in range(4)]
    return [exchange_blocks([cols[g][t] for g in range(4)], 1, 32) for t in range(4)]


def remap_back(grid):
    rows = [exchange_blocks(grid[t], 1, 32) for t in range(4)]
    cols = [exchange_blocks([rows[t][g] for t in range(4)], 0, 2) for g in range(4)]
    return [[cols[g][q] for g in range(4)] for q in range(4)]


class Plane:
    def __init__(self, ref, n):
        self.ref, self.n = ref, n

    def get(self, i, h):
        if i < 0:
            return pltpu.roll(self.ref[self.n - 1, h], 2, 0)
        if i >= self.n:
            return pltpu.roll(self.ref[0, h], 6, 0)
        return self.ref[i, h]

    def put(self, i, h, value):
        self.ref[i, h] = value


def neighbours(v, i, h, step, lane):
    own, other = v.get(i, h), v.get(i, 1 - h)
    below = pltpu.roll(jnp.where(lane >= 128 - step, other, own), step, 1)
    above = pltpu.roll(jnp.where(lane < step, other, own), 128 - step, 1)
    return (v.get(i - 1, h) + v.get(i + 1, h)) + (below + above)


def shifted_rows(a, edge, up):
    rows = a.shape[0]
    row = lax.broadcasted_iota(jnp.int32, a.shape, 0)
    if up:
        return jnp.where(row == rows - 1, edge, pltpu.roll(a, rows - 1, 0))
    return jnp.where(row == 0, edge, pltpu.roll(a, 1, 0))


def shifted_depth(a, up):
    depth = a.shape[1]
    col = lax.broadcasted_iota(jnp.int32, a.shape, 1)
    if up:
        return jnp.where(col == depth - 1, 0.0, pltpu.roll(a, depth - 1, 1))
    return jnp.where(col == 0, 0.0, pltpu.roll(a, 1, 1))


def transform(x, y, dim):
    return lax.dot_general(x, y, (((dim,), (dim,)), ((), ())), precision=HIGHEST, preferred_element_type=jnp.float32)


def coords(i):
    return (i // GY, lax.rem(i, GY))


def kernel(
    f_ref, p_ref, s_ref, st_ref, lam_hbm,
    pressure_ref, residual_ref,
    lam_ref, r_ref, o_ref, send, recv, back, e_ref, send_x, send_y, halo_x, halo_y,
    f0, f1, f2, f3, f4, a0, a1, a2, a3, a4, b0, b1, b2, b3, b4,
    lam_sem, hs_sem, hr_sem, s_sem, r_sem,
):
    gx, gy = lax.axis_index("gx"), lax.axis_index("gy")
    me = gx * GY + gy
    barrier = pltpu.get_barrier_semaphore()

    def greet(k, c):
        pl.semaphore_signal(barrier, inc=1, device_id=coords(lax.rem(me + k, NDEV)), device_id_type=MESH)
        return c

    lax.fori_loop(1, NDEV, greet, 0)
    lam_copy = pltpu.make_async_copy(lam_hbm.at[me], lam_ref, lam_sem)
    lam_copy.start()

    right, left = (lax.rem(gx + 1, GX), gy), (lax.rem(gx + GX - 1, GX), gy)
    upper, lower = (gx, lax.rem(gy + 1, GY)), (gx, lax.rem(gy + GY - 1, GY))

    def edge_copies(round_index):
        plan = ((send_x, halo_x, 0, right), (send_x, halo_x, 1, left), (send_y, halo_y, 0, upper), (send_y, halo_y, 1, lower))
        return [
            pltpu.make_async_remote_copy(
                source.at[round_index, side], target.at[round_index, side],
                hs_sem.at[round_index, n], hr_sem.at[round_index, n], device_id=to, device_id_type=MESH,
            )
            for n, (source, target, side, to) in enumerate(plan)
        ]

    send_x[0, 0] = f_ref[0, BX - 1] + p_ref[BX - 1]
    send_x[0, 1] = p_ref[0]
    for i in range(BX):
        send_y[0, 0, i] = f_ref[1, i, BY - 1] + p_ref[i, BY - 1]
        send_y[0, 1, i] = p_ref[i, 0]

    for i in range(BX):
        p, fx, fy, fz = p_ref[i], f_ref[0, i], f_ref[1, i], f_ref[2, i]
        r = shifted_depth(fz, False) - ((fx + fy + fz) + 4.0 * p)
        r = r + (shifted_rows(fy + p, 0.0, False) + shifted_rows(p, 0.0, True))
        if i > 0:
            r = r + (f_ref[0, i - 1] + p_ref[i - 1])
        if i < BX - 1:
            r = r + p_ref[i + 1]
        r_ref[i] = r

    pl.semaphore_wait(barrier, NDEV - 1)
    copies = edge_copies(0)
    for copy in copies:
        copy.start()
    for copy in copies:
        copy.wait()
    r_ref[0] = r_ref[0] + halo_x[0, 0]
    r_ref[BX - 1] = r_ref[BX - 1] + halo_x[0, 1]
    for i in range(BX):
        r_ref[i, 0] = r_ref[i, 0] + halo_y[0, 0, i]
        r_ref[i, BY - 1] = r_ref[i, BY - 1] + halo_y[0, 1, i]

    for t in range(4):
        rows = r_ref[4 * t : 4 * t + 4].reshape(128, NZ)
        flat = p_ref[4 * t : 4 * t + 4].reshape(128, NZ)
        o_ref[t] = transform(s_ref[...], rows, 1) + transform(st_ref[...], flat, 1)
    for g in range(32):
        parts = exchange_blocks([o_ref[t, 8 * g : 8 * g + 8] for t in range(4)], 0, 2)
        for j in range(4):
            send[4 * g + j] = parts[j]

    def all_to_all(target, which):
        def start(k, c):
            to = lax.rem(me + k, NDEV)
            pltpu.make_async_remote_copy(
                send.at[to], target.at[me], s_sem.at[which], r_sem.at[which], device_id=coords(to), device_id_type=MESH
            ).start()
            return c

        lax.fori_loop(1, NDEV, start, 0)
        target[me] = send[me]
        most = target.at[pl.ds(0, NDEV - 1)]
        pltpu.make_async_copy(most, most, r_sem.at[which]).wait()
        pltpu.make_async_copy(most, most, s_sem.at[which]).wait()

    all_to_all(recv, 0)
    lam_copy.wait()

    for gl in range(4):
        for h in range(2):
            grid = [[recv[(4 * q + gl) * GY + 4 * h + g] for g in range(4)] for q in range(4)]
            grid = remap(grid)
            for t in range(4):
                for x in range(4):
                    f0[16 * gl + 4 * t + x, h] = grid[t][x]

    lane = iota(1)
    lam = lam_ref[...]
    sizes = [64 >> level for level in range(LEVELS)]
    f = [Plane(ref, n) for ref, n in zip((f0, f1, f2, f3, f4), sizes)]
    a = [Plane(ref, n) for ref, n in zip((a0, a1, a2, a3, a4), sizes)]
    b = [Plane(ref, n) for ref, n in zip((b0, b1, b2, b3, b4), sizes)]

    def every(n):
        return ((i, h) for i in range(n) for h in range(2))

    def sweep(level, source, target):
        w = 0.25**level
        c = OMEGA / (4.0 * w + 2.0)
        keep = 1.0 - c * (4.0 * w + lam)
        for i, h in every(sizes[level]):
            beside = neighbours(source, i, h, 1 << level, lane)
            target.put(i, h, keep * source.get(i, h) + ((c * w) * beside + c * f[level].get(i, h)))

    def first_two(level, target):
        w = 0.25**level
        c = OMEGA / (4.0 * w + 2.0)
        keep = c * (2.0 - c * (4.0 * w + lam))
        for i, h in every(sizes[level]):
            beside = neighbours(f[level], i, h, 1 << level, lane)
            target.put(i, h, keep * f[level].get(i, h) + (c * c * w) * beside)

    def coarsen(level, source):
        w, step = 0.25**level, 1 << level
        first = lax.rem(lane // step, 2) == 0

        def rest(i, h):
            beside = neighbours(source, i, h, step, lane)
            own = source.get(i, h)
            return f[level].get(i, h) - (w * (4.0 * own - beside) + lam * own)

        for i, h in every(sizes[level + 1]):
            both = rest(2 * i, h) + rest(2 * i + 1, h)
            partner = jnp.where(first, pltpu.roll(both, 128 - step, 1), pltpu.roll(both, step, 1))
            f[level + 1].put(i, h, 0.25 * (both + partner))

    def correct(level, target, e):
        for i, h in every(sizes[level]):
            target.put(i, h, target.get(i, h) + e.get(i // 2, h))

    def coarsest(level):
        w = 0.25**level
        c = OMEGA / (4.0 * w + 2.0)
        total = functools.reduce(jnp.add, [f[level].get(i, h) for i, h in every(sizes[level])])
        total = total + pltpu.roll(total, 4, 0)
        total = total + pltpu.roll(total, 2, 0)
        mean = jnp.sum(total, axis=1, keepdims=True) * (1.0 / (2 * 4 * sizes[level] * 128))
        u = jnp.broadcast_to(mean, (8, 128)) / lam
        start = (1.0 - c * lam) * u
        for i, h in every(sizes[level]):
            a[level].put(i, h, start + c * f[level].get(i, h))
        sweep(level, a[level], b[level])
        sweep(level, b[level], a[level])
        sweep(level, a[level], b[level])
        return b[level]

    def cycle(level, first):
        if level == LEVELS - 1:
            return coarsest(level)
        if first:
            first_two(level, b[level])
        else:
            sweep(level, b[level], a[level])
            sweep(level, a[level], b[level])
        coarsen(level, b[level])
        e = cycle(level + 1, True)
        correct(level, b[level], e)
        sweep(level, b[level], a[level])
        sweep(level, a[level], b[level])
        return b[level]

    cycle(0, True)
    cycle(0, False)

    for gl in range(4):
        for h in range(2):
            grid = [[b0[16 * gl + 4 * t + x, h] for x in range(4)] for t in range(4)]
            grid = remap_back(grid)
            for q in range(4):
                for g in range(4):
                    send[(4 * q + gl) * GY + 4 * h + g] = grid[q][g]

    all_to_all(back, 1)

    for g in range(32):
        parts = exchange_blocks([back[4 * g + j] for j in range(4)], 0, 2)
        for t in range(4):
            o_ref[t, 8 * g : 8 * g + 8] = parts[t]
    for t in range(4):
        rows = transform(o_ref[t], s_ref[...], 0)
        e_ref[4 * t : 4 * t + 4] = rows.reshape(4, BY, NZ)

    send_x[1, 0] = e_ref[BX - 1]
    send_x[1, 1] = e_ref[0]
    for i in range(BX):
        send_y[1, 0, i] = e_ref[i, BY - 1]
        send_y[1, 1, i] = e_ref[i, 0]
    copies = edge_copies(1)
    for copy in copies:
        copy.start()
    for i in range(BX):
        e = e_ref[i]
        p = p_ref[i] + e
        pressure_ref[i] = p
        r = r_ref[i] - 4.0 * e + (shifted_depth(p, False) + shifted_depth(p, True) - 2.0 * p)
        r = r + (shifted_rows(e, 0.0, False) + shifted_rows(e, 0.0, True))
        if i > 0:
            r = r + e_ref[i - 1]
        if i < BX - 1:
            r = r + e_ref[i + 1]
        residual_ref[i] = r
    for copy in copies:
        copy.wait()
    residual_ref[0] = residual_ref[0] + halo_x[1, 0]
    residual_ref[BX - 1] = residual_ref[BX - 1] + halo_x[1, 1]
    for i in range(BX):
        residual_ref[i, 0] = residual_ref[i, 0] + halo_y[1, 0, i]
        residual_ref[i, BY - 1] = residual_ref[i, BY - 1] + halo_y[1, 1, i]


def on_device(forces, pressure_prev):
    block = (BX, BY, NZ)
    vmem = pl.BlockSpec(memory_space=pltpu.VMEM)
    levels = [pltpu.VMEM((64 >> level, 2, 8, 128), jnp.float32) for level in range(LEVELS)]
    return pl.pallas_call(
        kernel,
        out_shape=(jax.ShapeDtypeStruct(block, jnp.float32), jax.ShapeDtypeStruct(block, jnp.float32)),
        in_specs=[vmem, vmem, vmem, vmem, pl.BlockSpec(memory_space=pl.ANY)],
        out_specs=(vmem, vmem),
        scratch_shapes=[
            pltpu.VMEM((8, 128), jnp.float32),
            pltpu.VMEM(block, jnp.float32),
            pltpu.VMEM((4, NZ, 128), jnp.float32),
            pltpu.VMEM((NDEV, 8, 128), jnp.float32),
            pltpu.VMEM((NDEV, 8, 128), jnp.float32),
            pltpu.VMEM((NDEV, 8, 128), jnp.float32),
            pltpu.VMEM(block, jnp.float32),
            pltpu.VMEM((2, 2, BY, NZ), jnp.float32),
            pltpu.VMEM((2, 2, BX, NZ), jnp.float32),
            pltpu.VMEM((2, 2, BY, NZ), jnp.float32),
            pltpu.VMEM((2, 2, BX, NZ), jnp.float32),
            *levels, *levels, *levels,
            pltpu.SemaphoreType.DMA,
            pltpu.SemaphoreType.DMA((2, 4)),
            pltpu.SemaphoreType.DMA((2, 4)),
            pltpu.SemaphoreType.DMA((2,)),
            pltpu.SemaphoreType.DMA((2,)),
        ],
        compiler_params=pltpu.CompilerParams(collective_id=0, has_side_effects=True),
        name="poisson",
    )(
        forces,
        pressure_prev,
        jnp.asarray(sine_matrix()),
        jnp.asarray(sine_matrix(-spectrum()[:, None])),
        jnp.asarray(eigenvalues()),
    )


def solution(mesh):
    return jax.shard_map(
        on_device,
        mesh=mesh,
        in_specs=(P(None, "gx", "gy", None), P("gx", "gy", None)),
        out_specs=(P("gx", "gy", None), P("gx", "gy", None)),
        check_vma=False,
    )
```

```python
import contextlib
import functools

import jax
import jax.numpy as jnp
import numpy as np
from jax import lax
from jax.experimental import pallas as pl
from jax.experimental.pallas import tpu as pltpu
from jax.sharding import PartitionSpec as P

MESH = pl.DeviceIdType.MESH
OMEGA = 0.8
LEVELS = 5
GX, GY = 16, 8
NDEV = GX * GY
BX, BY, NZ = 16, 32, 256
TILES = 5
ROWS = 2 * TILES
HIGHEST = lax.Precision.HIGHEST
SCOPES = False


def scope(name):
    return jax.named_scope(name) if SCOPES else contextlib.nullcontext()


def spectrum():
    k = np.arange(1, NZ + 1, dtype=np.float64)
    return 4.0 * np.sin(0.5 * np.pi * k / (NZ + 1)) ** 2


def sine_matrix(weight=1.0):
    k = np.arange(1, NZ + 1, dtype=np.float64)
    return (weight * (np.sqrt(2.0 / (NZ + 1)) * np.sin(np.pi * np.outer(k, k) / (NZ + 1)))).astype(np.float32)


def eigenvalues():
    rows = np.tile(spectrum().reshape(NDEV, 2), (1, 4))
    return np.broadcast_to(rows[:, :, None], (NDEV, 8, 128)).astype(np.float32)


def iota(axis):
    return lax.broadcasted_iota(jnp.int32, (8, 128), axis)


def shifted_rows(a, up):
    rows = a.shape[0]
    row = lax.broadcasted_iota(jnp.int32, a.shape, 0)
    if up:
        return jnp.where(row == rows - 1, 0.0, pltpu.roll(a, rows - 1, 0))
    return jnp.where(row == 0, 0.0, pltpu.roll(a, 1, 0))


def shifted_depth(a, up):
    depth = a.shape[1]
    col = lax.broadcasted_iota(jnp.int32, a.shape, 1)
    if up:
        return jnp.where(col == depth - 1, 0.0, pltpu.roll(a, depth - 1, 1))
    return jnp.where(col == 0, 0.0, pltpu.roll(a, 1, 1))


def transform(x, y, dim):
    return lax.dot_general(x, y, (((dim,), (dim,)), ((), ())), precision=HIGHEST, preferred_element_type=jnp.float32)


def fence():
    pl.delay(1)


class Lanes:
    def __init__(self):
        gx = lax.rem(iota(1), GX)
        self.first, self.last = gx == 0, gx == GX - 1
        self.sub = iota(0)

    def from_left(self, v):
        return jnp.where(self.first, pltpu.roll(v, 128 - (GX - 1), 1), pltpu.roll(v, 1, 1))

    def from_right(self, v):
        return jnp.where(self.last, pltpu.roll(v, GX - 1, 1), pltpu.roll(v, 127, 1))

    def from_below(self, v):
        return pltpu.roll(v, GX, 1)

    def from_above(self, v):
        return pltpu.roll(v, 128 - GX, 1)


class Field:
    def __init__(self, level, ref=None):
        self.level, self.ref, self.held = level, ref, {}
        self.nx, self.ny = BX >> level, max(1, 4 >> level)
        self.step = max(1, (1 << level) // 4)

    def cells(self):
        return [(x, y) for x in range(self.nx) for y in range(self.ny)]

    def get(self, x, y):
        return self.held[x, y] if self.ref is None else self.ref[x, y]

    def put(self, x, y, value):
        if self.ref is None:
            self.held[x, y] = value
        else:
            self.ref[x, y] = value

    def beside(self, x, y, lanes):
        step = self.step
        left = self.get(x - 1, y) if x > 0 else lanes.from_left(self.get(self.nx - 1, y))
        right = self.get(x + 1, y) if x < self.nx - 1 else lanes.from_right(self.get(0, y))
        if y > 0:
            below = self.get(x, y - 1)
        else:
            below = pltpu.roll(self.get(x, self.ny - 1), step, 0)
            below = jnp.where(lanes.sub < step, lanes.from_below(below), below)
        if y < self.ny - 1:
            above = self.get(x, y + 1)
        else:
            above = pltpu.roll(self.get(x, 0), 8 - step, 0)
            above = jnp.where(lanes.sub >= 8 - step, lanes.from_above(above), above)
        return (left + right) + (below + above)


def weights(level):
    w = 0.25**level
    return w, OMEGA / (4.0 * w + 2.0)


def sweep(source, f, target, lam, lanes):
    w, c = weights(source.level)
    keep = 1.0 - c * (4.0 * w + lam)
    for x, y in source.cells():
        beside = source.beside(x, y, lanes)
        target.put(x, y, keep * source.get(x, y) + ((c * w) * beside + c * f.get(x, y)))


def first_two(f, target, lam, lanes):
    w, c = weights(f.level)
    keep = c * (2.0 - c * (4.0 * w + lam))
    for x, y in f.cells():
        target.put(x, y, keep * f.get(x, y) + (c * c * w) * f.beside(x, y, lanes))


def coarsen(source, f, coarse, lam, lanes):
    w, _ = weights(source.level)

    def rest(x, y):
        own = source.get(x, y)
        return f.get(x, y) - (w * (4.0 * own - source.beside(x, y, lanes)) + lam * own)

    for x, y in coarse.cells():
        if source.ny > 1:
            total = (rest(2 * x, 2 * y) + rest(2 * x + 1, 2 * y)) + (rest(2 * x, 2 * y + 1) + rest(2 * x + 1, 2 * y + 1))
        else:
            step = source.step
            both = rest(2 * x, y) + rest(2 * x + 1, y)
            even = lax.rem(lanes.sub // step, 2) == 0
            total = both + jnp.where(even, pltpu.roll(both, 8 - step, 0), pltpu.roll(both, step, 0))
        coarse.put(x, y, 0.25 * total)


def correct(target, e):
    for x, y in target.cells():
        target.put(x, y, target.get(x, y) + e.get(x // 2, y // 2 if target.ny > 1 else 0))


def coarsest(f, lam, lanes):
    level = f.level
    _, c = weights(level)
    own = f.get(0, 0)
    total = jnp.broadcast_to(jnp.sum(own, axis=1, keepdims=True), (8, 128))
    total = total + pltpu.roll(total, 4, 0)
    total = total + pltpu.roll(total, 2, 0)
    total = total + pltpu.roll(total, 1, 0)
    u = (total * (1.0 / 1024.0)) / lam
    v = Field(level)
    v.put(0, 0, (1.0 - c * lam) * u + c * own)
    for _ in range(3):
        new = Field(level)
        sweep(v, f, new, lam, lanes)
        v = new
    return v


def kernel(
    f_hbm, p_hbm, s_hbm, st_hbm, lam_hbm,
    pressure_hbm, residual_hbm,
    f_ref, p_ref, s_ref, st_ref, lam_ref, r_ref, g_ref, o_ref, e_ref, ends_ref, pressure_ref, residual_ref,
    send, recv, reply, back, w_ref, row_ref, f0, a0, b0, f1, a1, b1,
    in_sem, out_sem, s_sem, r_sem,
):
    gx, gy = lax.axis_index("gx"), lax.axis_index("gy")
    me = gy * GX + gx
    loads = [
        pltpu.make_async_copy(source, target, in_sem.at[n])
        for n, (source, target) in enumerate(
            ((f_hbm, f_ref), (p_hbm, p_ref), (s_hbm, s_ref), (st_hbm, st_ref), (lam_hbm.at[me], lam_ref))
        )
    ]
    for load in loads:
        load.start()

    to_x = [lax.rem(gx + a, GX) for a in range(GX)]

    def partners(visit):
        for a in range(1, GX):
            visit(to_x[a], gy)

        def row(b, c):
            y = lax.rem(gy + b, GY)
            for a in range(GX):
                visit(to_x[a], y)
            return c

        lax.fori_loop(1, GY, row, 0)

    barrier = pltpu.get_barrier_semaphore()
    with scope("greet"):
        partners(lambda x, y: pl.semaphore_signal(barrier, inc=1, device_id=(x, y), device_id_type=MESH))
    with scope("load"):
        for load in loads:
            load.wait()

    with scope("stage_a"):
        g_ref[0:32] = f_ref[0, BX - 1] + p_ref[BX - 1]
        g_ref[32:64] = p_ref[0]
        g_ref[96:128] = jnp.zeros((32, NZ), jnp.float32)
        for i in range(BX):
            p, fx, fy, fz = p_ref[i], f_ref[0, i], f_ref[1, i], f_ref[2, i]
            r = shifted_depth(fz, False) - ((fx + fy + fz) + 4.0 * p)
            r = r + (shifted_rows(fy + p, False) + shifted_rows(p, True))
            if i > 0:
                r = r + (f_ref[0, i - 1] + p_ref[i - 1])
            if i < BX - 1:
                r = r + p_ref[i + 1]
            r_ref[i] = r
            g_ref[64 + i] = f_ref[1, i, BY - 1] + p_ref[i, BY - 1]
            g_ref[80 + i] = p_ref[i, 0]

    with scope("dst"):
        for t in range(4):
            rows = r_ref[4 * t : 4 * t + 4].reshape(128, NZ)
            flat = p_ref[4 * t : 4 * t + 4].reshape(128, NZ)
            o_ref[t] = transform(s_ref[...], rows, 1) + transform(st_ref[...], flat, 1)
        o_ref[4] = transform(s_ref[...], g_ref[...], 1)
    with scope("pack"):
        for t in range(TILES):
            for k in range(2):
                send[pl.ds(2 * t + k, NDEV, stride=ROWS), :] = o_ref[t, pl.ds(k, NDEV, stride=2), :]

    with scope("barrier"):
        pl.semaphore_wait(barrier, NDEV - 1)

    def blocks(ref, index):
        return ref.at[pl.ds(index * ROWS, ROWS)]

    def start_all_to_all(source, target, which):
        mine = blocks(target, me)

        def visit(x, y):
            pltpu.make_async_remote_copy(
                blocks(source, y * GX + x), mine, s_sem.at[which], r_sem.at[which], device_id=(x, y), device_id_type=MESH
            ).start()

        partners(visit)
        target[pl.ds(me * ROWS, ROWS), :] = source[pl.ds(me * ROWS, ROWS), :]

    def wait_all(ref, sem):
        most = ref.at[pl.ds(0, (NDEV - 1) * ROWS)]
        pltpu.make_async_copy(most, most, sem).wait()

    with scope("a2a_1_start"):
        start_all_to_all(send, recv, 0)
    with scope("a2a_1_wait"):
        wait_all(recv, r_sem.at[0])

    lanes = Lanes()
    with scope("unpack"):
        for n in range(ROWS):
            w_ref[n] = recv[pl.ds(n, NDEV, stride=ROWS), :].T
        for k in range(2):
            for half in range(2):
                at = 8 * half
                row_ref[k, at : at + 8] = lanes.from_below(w_ref[8 + k, 64 + at : 72 + at])
                row_ref[k, 16 + at : 24 + at] = lanes.from_above(w_ref[8 + k, 80 + at : 88 + at])
        for k in range(2):
            for x in range(BX):
                t, x4 = divmod(x, 4)
                for y in range(4):
                    value = w_ref[2 * t + k, pl.ds(32 * x4 + y, 8, stride=4), :]
                    if x == 0:
                        value = value + lanes.from_left(w_ref[8 + k, pl.ds(y, 8, stride=4), :])
                    if x == BX - 1:
                        value = value + lanes.from_right(w_ref[8 + k, pl.ds(32 + y, 8, stride=4), :])
                    if y == 0:
                        value = value + jnp.where(lanes.sub == 0, row_ref[k, x : x + 1], 0.0)
                    if y == 3:
                        value = value + jnp.where(lanes.sub == 7, row_ref[k, 16 + x : 17 + x], 0.0)
                    f0[k, x, y] = value

    lams = [jnp.broadcast_to(lam_ref[k : k + 1], (8, 128)) for k in range(2)]

    def both(step):
        for k in range(2):
            step(k)
        fence()

    fields = [[(Field(0, f0.at[k]), Field(0, a0.at[k]), Field(0, b0.at[k])) for k in range(2)],
              [(Field(1, f1.at[k]), Field(1, a1.at[k]), Field(1, b1.at[k])) for k in range(2)]]

    def small(f, lam):
        level = f.level
        if level == LEVELS - 1:
            return coarsest(f, lam, lanes)
        v, coarse = Field(level), Field(level + 1)
        first_two(f, v, lam, lanes)
        coarsen(v, f, coarse, lam, lanes)
        correct(v, small(coarse, lam))
        for _ in range(2):
            new = Field(level)
            sweep(v, f, new, lam, lanes)
            v = new
        return v

    def cycle(level, first):
        def parts(k):
            return fields[level][k]

        def named(name, step):
            with scope(f"{name}_{level}"):
                both(step)

        if first:
            named("first_two", lambda k: first_two(parts(k)[0], parts(k)[2], lams[k], lanes))
        else:
            named("sweep", lambda k: sweep(parts(k)[2], parts(k)[0], parts(k)[1], lams[k], lanes))
            named("sweep", lambda k: sweep(parts(k)[1], parts(k)[0], parts(k)[2], lams[k], lanes))
        if level == 0:
            named("coarsen", lambda k: coarsen(parts(k)[2], parts(k)[0], fields[1][k][0], lams[k], lanes))
            cycle(1, True)
            named("correct", lambda k: correct(parts(k)[2], fields[1][k][2]))
        else:
            def inner(k):
                coarse = Field(2)
                coarsen(parts(k)[2], parts(k)[0], coarse, lams[k], lanes)
                correct(parts(k)[2], small(coarse, lams[k]))

            named("inner", inner)
        named("sweep", lambda k: sweep(parts(k)[2], parts(k)[0], parts(k)[1], lams[k], lanes))
        named("sweep", lambda k: sweep(parts(k)[1], parts(k)[0], parts(k)[2], lams[k], lanes))

    cycle(0, True)
    cycle(0, False)

    with scope("repack"):
        for k in range(2):
            edge = w_ref.at[8 + k]
            for y in range(4):
                low = edge[pl.ds(y, 8, stride=4), :] + b0[k, BX - 1, y]
                high = edge[pl.ds(32 + y, 8, stride=4), :] + b0[k, 0, y]
                edge[pl.ds(y, 8, stride=4), :] = lanes.from_left(low)
                edge[pl.ds(32 + y, 8, stride=4), :] = lanes.from_right(high)
            for x in range(BX):
                edge[64 + x : 65 + x, :] = row_ref[k, x : x + 1] + lanes.from_below(b0[k, x, 3])[7:8]
                edge[80 + x : 81 + x, :] = row_ref[k, 16 + x : 17 + x] + lanes.from_above(b0[k, x, 0])[0:1]
                t, x4 = divmod(x, 4)
                for y in range(4):
                    w_ref[2 * t + k, pl.ds(32 * x4 + y, 8, stride=4), :] = b0[k, x, y]
        fence()
        for n in range(ROWS):
            reply[pl.ds(n, NDEV, stride=ROWS), :] = w_ref[n].T

    with scope("a2a_2_start"):
        start_all_to_all(reply, back, 1)
    with scope("a2a_2_wait"):
        wait_all(back, r_sem.at[1])

    with scope("idst"):
        for t in range(TILES):
            for k in range(2):
                o_ref[t, pl.ds(k, NDEV, stride=2), :] = back[pl.ds(2 * t + k, NDEV, stride=ROWS), :]
        for t in range(4):
            e_ref[4 * t : 4 * t + 4] = transform(o_ref[t], s_ref[...], 0).reshape(4, BY, NZ)
        ends_ref[...] = transform(o_ref[4], s_ref[...], 0)

    with scope("final"):
        for i in range(BX):
            e = e_ref[i]
            p = p_ref[i] + e
            pressure_ref[i] = p
            r = r_ref[i] - 4.0 * e + (shifted_depth(p, False) + shifted_depth(p, True) - 2.0 * p)
            r = r + (shifted_rows(e, False) + shifted_rows(e, True))
            r = r + (e_ref[i - 1] if i > 0 else ends_ref[0:32])
            r = r + (e_ref[i + 1] if i < BX - 1 else ends_ref[32:64])
            residual_ref[i] = r
            residual_ref[i, 0] = residual_ref[i, 0] + ends_ref[64 + i]
            residual_ref[i, BY - 1] = residual_ref[i, BY - 1] + ends_ref[80 + i]

    with scope("store"):
        stores = [
            pltpu.make_async_copy(source, target, out_sem.at[n])
            for n, (source, target) in enumerate(((pressure_ref, pressure_hbm), (residual_ref, residual_hbm)))
        ]
        for store in stores:
            store.start()
        wait_all(send, s_sem.at[0])
        wait_all(reply, s_sem.at[1])
        for store in stores:
            store.wait()


def on_device(forces, pressure_prev):
    block = (BX, BY, NZ)
    anywhere = pl.BlockSpec(memory_space=pl.ANY)

    def vmem(*shape):
        return pltpu.VMEM(shape, jnp.float32)

    return pl.pallas_call(
        kernel,
        out_shape=(jax.ShapeDtypeStruct(block, jnp.float32), jax.ShapeDtypeStruct(block, jnp.float32)),
        in_specs=[anywhere] * 5,
        out_specs=(anywhere, anywhere),
        scratch_shapes=[
            vmem(3, *block), vmem(*block), vmem(NZ, NZ), vmem(NZ, NZ), vmem(8, 128),
            vmem(*block), vmem(128, NZ), vmem(TILES, NZ, 128), vmem(*block), vmem(128, NZ), vmem(*block), vmem(*block),
            vmem(NDEV * ROWS, 128), vmem(NDEV * ROWS, 128), vmem(NDEV * ROWS, 128), vmem(NDEV * ROWS, 128),
            vmem(ROWS, 128, 128), vmem(2, 32, 128),
            *[vmem(2, 16, 4, 8, 128)] * 3, *[vmem(2, 8, 2, 8, 128)] * 3,
            pltpu.SemaphoreType.DMA((5,)),
            pltpu.SemaphoreType.DMA((2,)),
            pltpu.SemaphoreType.DMA((2,)),
            pltpu.SemaphoreType.DMA((2,)),
        ],
        compiler_params=pltpu.CompilerParams(collective_id=0, has_side_effects=True),
        name="poisson",
    )(
        forces,
        pressure_prev,
        jnp.asarray(sine_matrix()),
        jnp.asarray(sine_matrix(-spectrum()[:, None])),
        jnp.asarray(eigenvalues()),
    )


def solution(mesh):
    return jax.shard_map(
        on_device,
        mesh=mesh,
        in_specs=(P(None, "gx", "gy", None), P("gx", "gy", None)),
        out_specs=(P("gx", "gy", None), P("gx", "gy", None)),
        check_vma=False,
    )
```

```python
import contextlib
import functools

import jax
import jax.numpy as jnp
import numpy as np
from jax import lax
from jax.experimental import pallas as pl
from jax.experimental.pallas import tpu as pltpu
from jax.sharding import PartitionSpec as P

MESH = pl.DeviceIdType.MESH
OMEGA = 0.8
LEVELS = 5
GX, GY = 16, 8
NDEV = GX * GY
BX, BY, NZ = 16, 32, 256
TILES = 5
HIGHEST = lax.Precision.HIGHEST
SCOPES = False


def scope(name):
    return jax.named_scope(name) if SCOPES else contextlib.nullcontext()


def spectrum():
    k = np.arange(1, NZ + 1, dtype=np.float64)
    return 4.0 * np.sin(0.5 * np.pi * k / (NZ + 1)) ** 2


def sine_matrix(weight=1.0):
    k = np.arange(1, NZ + 1, dtype=np.float64)
    full = weight * (np.sqrt(2.0 / (NZ + 1)) * np.sin(np.pi * np.outer(k, k) / (NZ + 1)))
    return np.concatenate([full[0::2], full[1::2]]).astype(np.float32)


def eigenvalues():
    rows = np.tile(spectrum().reshape(NDEV, 2), (1, 4))
    return np.broadcast_to(rows[:, :, None], (NDEV, 8, 128)).astype(np.float32)


def iota(axis):
    return lax.broadcasted_iota(jnp.int32, (8, 128), axis)


def shifted_rows(a, up):
    rows = a.shape[0]
    row = lax.broadcasted_iota(jnp.int32, a.shape, 0)
    if up:
        return jnp.where(row == rows - 1, 0.0, pltpu.roll(a, rows - 1, 0))
    return jnp.where(row == 0, 0.0, pltpu.roll(a, 1, 0))


def shifted_depth(a, up):
    depth = a.shape[1]
    col = lax.broadcasted_iota(jnp.int32, a.shape, 1)
    if up:
        return jnp.where(col == depth - 1, 0.0, pltpu.roll(a, depth - 1, 1))
    return jnp.where(col == 0, 0.0, pltpu.roll(a, 1, 1))


def transform(x, y, dim):
    return lax.dot_general(x, y, (((dim,), (dim,)), ((), ())), precision=HIGHEST, preferred_element_type=jnp.float32)


def fence():
    pl.delay(1)


class Lanes:
    def __init__(self):
        gx = lax.rem(iota(1), GX)
        self.first, self.last = gx == 0, gx == GX - 1
        self.sub = iota(0)

    def from_left(self, v):
        return jnp.where(self.first, pltpu.roll(v, 128 - (GX - 1), 1), pltpu.roll(v, 1, 1))

    def from_right(self, v):
        return jnp.where(self.last, pltpu.roll(v, GX - 1, 1), pltpu.roll(v, 127, 1))

    def from_below(self, v):
        return pltpu.roll(v, GX, 1)

    def from_above(self, v):
        return pltpu.roll(v, 128 - GX, 1)


class Field:
    def __init__(self, level, ref=None):
        self.level, self.ref, self.held = level, ref, {}
        self.nx, self.ny = BX >> level, max(1, 4 >> level)
        self.step = max(1, (1 << level) // 4)

    def cells(self):
        return [(x, y) for x in range(self.nx) for y in range(self.ny)]

    def get(self, x, y):
        return self.held[x, y] if self.ref is None else self.ref[x, y]

    def put(self, x, y, value):
        if self.ref is None:
            self.held[x, y] = value
        else:
            self.ref[x, y] = value

    def beside(self, x, y, lanes):
        step = self.step
        left = self.get(x - 1, y) if x > 0 else lanes.from_left(self.get(self.nx - 1, y))
        right = self.get(x + 1, y) if x < self.nx - 1 else lanes.from_right(self.get(0, y))
        if y > 0:
            below = self.get(x, y - 1)
        else:
            below = pltpu.roll(self.get(x, self.ny - 1), step, 0)
            below = jnp.where(lanes.sub < step, lanes.from_below(below), below)
        if y < self.ny - 1:
            above = self.get(x, y + 1)
        else:
            above = pltpu.roll(self.get(x, 0), 8 - step, 0)
            above = jnp.where(lanes.sub >= 8 - step, lanes.from_above(above), above)
        return (left + right) + (below + above)


def weights(level):
    w = 0.25**level
    return w, OMEGA / (4.0 * w + 2.0)


def sweep(source, f, target, lam, lanes):
    w, c = weights(source.level)
    keep = 1.0 - c * (4.0 * w + lam)
    for x, y in source.cells():
        beside = source.beside(x, y, lanes)
        target.put(x, y, keep * source.get(x, y) + ((c * w) * beside + c * f.get(x, y)))


def first_two(f, target, lam, lanes):
    w, c = weights(f.level)
    keep = c * (2.0 - c * (4.0 * w + lam))
    for x, y in f.cells():
        target.put(x, y, keep * f.get(x, y) + (c * c * w) * f.beside(x, y, lanes))


def coarsen(source, f, coarse, lam, lanes):
    w, _ = weights(source.level)

    def rest(x, y):
        own = source.get(x, y)
        return f.get(x, y) - (w * (4.0 * own - source.beside(x, y, lanes)) + lam * own)

    for x, y in coarse.cells():
        if source.ny > 1:
            total = (rest(2 * x, 2 * y) + rest(2 * x + 1, 2 * y)) + (rest(2 * x, 2 * y + 1) + rest(2 * x + 1, 2 * y + 1))
        else:
            step = source.step
            both = rest(2 * x, y) + rest(2 * x + 1, y)
            even = lax.rem(lanes.sub // step, 2) == 0
            total = both + jnp.where(even, pltpu.roll(both, 8 - step, 0), pltpu.roll(both, step, 0))
        coarse.put(x, y, 0.25 * total)


def correct(target, e):
    for x, y in target.cells():
        target.put(x, y, target.get(x, y) + e.get(x // 2, y // 2 if target.ny > 1 else 0))


def coarsest(f, lam, lanes):
    level = f.level
    _, c = weights(level)
    own = f.get(0, 0)
    total = jnp.broadcast_to(jnp.sum(own, axis=1, keepdims=True), (8, 128))
    total = total + pltpu.roll(total, 4, 0)
    total = total + pltpu.roll(total, 2, 0)
    total = total + pltpu.roll(total, 1, 0)
    u = (total * (1.0 / 1024.0)) / lam
    v = Field(level)
    v.put(0, 0, (1.0 - c * lam) * u + c * own)
    for _ in range(3):
        new = Field(level)
        sweep(v, f, new, lam, lanes)
        v = new
    return v


def kernel(
    f_hbm, p_hbm, s_hbm, st_hbm, lam_hbm,
    pressure_ref, residual_ref,
    f_ref, p_ref, s_ref, st_ref, lam_ref, r_ref, g_ref, o_ref, e_ref,
    send, recv, reply, back, w_ref, row_ref, f0, a0, b0, f1, a1, b1,
    in_sem, s_sem, r_sem,
):
    gx, gy = lax.axis_index("gx"), lax.axis_index("gy")
    me = gy * GX + gx
    loads = [
        pltpu.make_async_copy(source, target, in_sem.at[n])
        for n, (source, target) in enumerate(
            ((f_hbm, f_ref), (p_hbm, p_ref), (s_hbm, s_ref), (st_hbm, st_ref), (lam_hbm.at[me], lam_ref))
        )
    ]
    for load in loads:
        load.start()

    to_x = [lax.rem(gx + a, GX) for a in range(GX)]

    def partners(visit):
        for a in range(1, GX):
            visit(to_x[a], gy)

        def row(b, c):
            y = lax.rem(gy + b, GY)
            for a in range(GX):
                visit(to_x[a], y)
            return c

        lax.fori_loop(1, GY, row, 0)

    barrier = pltpu.get_barrier_semaphore()
    with scope("greet"):
        partners(lambda x, y: pl.semaphore_signal(barrier, inc=1, device_id=(x, y), device_id_type=MESH))
    with scope("load"):
        for load in loads:
            load.wait()

    with scope("stage_a"):
        g_ref[0:32] = f_ref[0, BX - 1] + p_ref[BX - 1]
        g_ref[32:64] = p_ref[0]
        g_ref[96:128] = jnp.zeros((32, NZ), jnp.float32)
        for i in range(BX):
            p, fx, fy, fz = p_ref[i], f_ref[0, i], f_ref[1, i], f_ref[2, i]
            r = shifted_depth(fz, False) - ((fx + fy + fz) + 4.0 * p)
            r = r + (shifted_rows(fy + p, False) + shifted_rows(p, True))
            if i > 0:
                r = r + (f_ref[0, i - 1] + p_ref[i - 1])
            if i < BX - 1:
                r = r + p_ref[i + 1]
            r_ref[i] = r
            g_ref[64 + i] = f_ref[1, i, BY - 1] + p_ref[i, BY - 1]
            g_ref[80 + i] = p_ref[i, 0]

    with scope("dst"):
        for t in range(4):
            rows = r_ref[4 * t : 4 * t + 4].reshape(128, NZ)
            flat = p_ref[4 * t : 4 * t + 4].reshape(128, NZ)
            o_ref[t] = transform(s_ref[...], rows, 1) + transform(st_ref[...], flat, 1)
        o_ref[4] = transform(s_ref[...], g_ref[...], 1)
    with scope("pack"):
        for k in range(2):
            for t in range(TILES):
                send[k, pl.ds(t, NDEV, stride=TILES), :] = o_ref[t, k * NDEV : (k + 1) * NDEV]

    with scope("barrier"):
        pl.semaphore_wait(barrier, NDEV - 1)

    def start_all_to_all(source, target, which):
        mine = target.at[pl.ds(me * TILES, TILES)]

        def visit(x, y):
            pltpu.make_async_remote_copy(
                source.at[pl.ds((y * GX + x) * TILES, TILES)], mine, s_sem.at[which], r_sem.at[which],
                device_id=(x, y), device_id_type=MESH,
            ).start()

        partners(visit)
        target[pl.ds(me * TILES, TILES), :] = source[pl.ds(me * TILES, TILES), :]

    def wait_all(ref, sem):
        most = ref.at[pl.ds(0, (NDEV - 1) * TILES)]
        pltpu.make_async_copy(most, most, sem).wait()

    with scope("a2a_1_start"):
        for k in range(2):
            start_all_to_all(send.at[k], recv.at[k], k)

    lanes = Lanes()

    def unpack(k):
        w = w_ref.at[k]
        for n in range(TILES):
            w[n] = recv[k, pl.ds(n, NDEV, stride=TILES), :].T
        for half in range(2):
            at = 8 * half
            row_ref[k, at : at + 8] = lanes.from_below(w[4, 64 + at : 72 + at])
            row_ref[k, 16 + at : 24 + at] = lanes.from_above(w[4, 80 + at : 88 + at])
        for x in range(BX):
            t, x4 = divmod(x, 4)
            for y in range(4):
                value = w[t, pl.ds(32 * x4 + y, 8, stride=4), :]
                if x == 0:
                    value = value + lanes.from_left(w[4, pl.ds(y, 8, stride=4), :])
                if x == BX - 1:
                    value = value + lanes.from_right(w[4, pl.ds(32 + y, 8, stride=4), :])
                if y == 0:
                    value = value + jnp.where(lanes.sub == 0, row_ref[k, x : x + 1], 0.0)
                if y == 3:
                    value = value + jnp.where(lanes.sub == 7, row_ref[k, 16 + x : 17 + x], 0.0)
                f0[k, x, y] = value

    lams = [jnp.broadcast_to(lam_ref[k : k + 1], (8, 128)) for k in range(2)]

    fields = [[(Field(0, f0.at[k]), Field(0, a0.at[k]), Field(0, b0.at[k])) for k in range(2)],
              [(Field(1, f1.at[k]), Field(1, a1.at[k]), Field(1, b1.at[k])) for k in range(2)]]

    def small(f, lam):
        level = f.level
        if level == LEVELS - 1:
            return coarsest(f, lam, lanes)
        v, coarse = Field(level), Field(level + 1)
        first_two(f, v, lam, lanes)
        coarsen(v, f, coarse, lam, lanes)
        correct(v, small(coarse, lam))
        for _ in range(2):
            new = Field(level)
            sweep(v, f, new, lam, lanes)
            v = new
        return v

    def cycle(k, level, first):
        f, a, b = fields[level][k]
        lam = lams[k]

        def named(name, step, *args):
            with scope(f"{name}_{level}"):
                step(*args, lam, lanes)
            fence()

        if first:
            named("first_two", first_two, f, b)
        else:
            named("sweep", sweep, b, f, a)
            named("sweep", sweep, a, f, b)
        if level == 0:
            named("coarsen", coarsen, b, f, fields[1][k][0])
            cycle(k, 1, True)
            named("correct", lambda v, e, *_: correct(v, e), b, fields[1][k][2])
        else:
            def inner(*_):
                coarse = Field(2)
                coarsen(b, f, coarse, lam, lanes)
                correct(b, small(coarse, lam))

            named("inner", inner)
        named("sweep", sweep, b, f, a)
        named("sweep", sweep, a, f, b)

    def repack(k):
        w = w_ref.at[k]
        edge = w.at[4]
        for y in range(4):
            low = edge[pl.ds(y, 8, stride=4), :] + b0[k, BX - 1, y]
            high = edge[pl.ds(32 + y, 8, stride=4), :] + b0[k, 0, y]
            edge[pl.ds(y, 8, stride=4), :] = lanes.from_left(low)
            edge[pl.ds(32 + y, 8, stride=4), :] = lanes.from_right(high)
        for x in range(BX):
            edge[64 + x : 65 + x, :] = row_ref[k, x : x + 1] + lanes.from_below(b0[k, x, 3])[7:8]
            edge[80 + x : 81 + x, :] = row_ref[k, 16 + x : 17 + x] + lanes.from_above(b0[k, x, 0])[0:1]
            t, x4 = divmod(x, 4)
            for y in range(4):
                w[t, pl.ds(32 * x4 + y, 8, stride=4), :] = b0[k, x, y]
        fence()
        for n in range(TILES):
            reply[k, pl.ds(n, NDEV, stride=TILES), :] = w[n].T

    for k in range(2):
        with scope(f"a2a_1_wait_{k}"):
            wait_all(recv.at[k], r_sem.at[k])
        with scope("unpack"):
            unpack(k)
        fence()
        cycle(k, 0, True)
        cycle(k, 0, False)
        with scope("repack"):
            repack(k)
        with scope("a2a_2_start"):
            start_all_to_all(reply.at[k], back.at[k], 2 + k)

    for k in range(2):
        with scope(f"a2a_2_wait_{k}"):
            wait_all(back.at[k], r_sem.at[2 + k])
        with scope("idst"):
            basis = s_ref[k * NDEV : (k + 1) * NDEV]
            for t in range(TILES):
                part = transform(back[k, pl.ds(t, NDEV, stride=TILES), :], basis, 0)
                e_ref[t] = part if k == 0 else e_ref[t] + part

    def plane(i):
        return e_ref[i // 4, 32 * (i % 4) : 32 * (i % 4) + 32]

    with scope("final"):
        for i in range(BX):
            e = plane(i)
            p = p_ref[i] + e
            pressure_ref[i] = p
            r = r_ref[i] - 4.0 * e + (shifted_depth(p, False) + shifted_depth(p, True) - 2.0 * p)
            r = r + (shifted_rows(e, False) + shifted_rows(e, True))
            r = r + (plane(i - 1) if i > 0 else e_ref[4, 0:32])
            r = r + (plane(i + 1) if i < BX - 1 else e_ref[4, 32:64])
            residual_ref[i] = r
            residual_ref[i, 0] = residual_ref[i, 0] + e_ref[4, 64 + i]
            residual_ref[i, BY - 1] = residual_ref[i, BY - 1] + e_ref[4, 80 + i]

    with scope("drain"):
        for k in range(2):
            wait_all(send.at[k], s_sem.at[k])
            wait_all(reply.at[k], s_sem.at[2 + k])


def on_device(forces, pressure_prev):
    block = (BX, BY, NZ)
    anywhere = pl.BlockSpec(memory_space=pl.ANY)

    def vmem(*shape):
        return pltpu.VMEM(shape, jnp.float32)

    return pl.pallas_call(
        kernel,
        out_shape=(pltpu.VMEM(block, jnp.float32), pltpu.VMEM(block, jnp.float32)),
        in_specs=[anywhere] * 5,
        out_specs=(pl.BlockSpec(memory_space=pltpu.VMEM),) * 2,
        scratch_shapes=[
            vmem(3, *block), vmem(*block), vmem(NZ, NZ), vmem(NZ, NZ), vmem(8, 128),
            vmem(*block), vmem(128, NZ), vmem(TILES, NZ, 128), vmem(TILES, 128, NZ),
            *[vmem(2, NDEV * TILES, 128)] * 4, vmem(2, TILES, 128, 128), vmem(2, 32, 128),
            *[vmem(2, 16, 4, 8, 128)] * 3, *[vmem(2, 8, 2, 8, 128)] * 3,
            pltpu.SemaphoreType.DMA((5,)),
            pltpu.SemaphoreType.DMA((4,)),
            pltpu.SemaphoreType.DMA((4,)),
        ],
        compiler_params=pltpu.CompilerParams(collective_id=0, has_side_effects=True),
        name="poisson",
    )(
        forces,
        pressure_prev,
        jnp.asarray(sine_matrix()),
        jnp.asarray(sine_matrix(-spectrum()[:, None])),
        jnp.asarray(eigenvalues()),
    )


def solution(mesh):
    return jax.shard_map(
        on_device,
        mesh=mesh,
        in_specs=(P(None, "gx", "gy", None), P("gx", "gy", None)),
        out_specs=(P("gx", "gy", None), P("gx", "gy", None)),
        check_vma=False,
    )
```

```python
import contextlib
import functools

import jax
import jax.numpy as jnp
import numpy as np
from jax import lax
from jax.experimental import pallas as pl
from jax.experimental.pallas import tpu as pltpu
from jax.sharding import PartitionSpec as P

MESH = pl.DeviceIdType.MESH
OMEGA = 0.8
LEVELS = 5
GX, GY = 16, 8
NDEV = GX * GY
BX, BY, NZ = 16, 32, 256
TILES = 5
HIGHEST = lax.Precision.HIGHEST
SCOPES = False
PAUSE = 3600


def steps(distance, size):
    return min(distance, size - distance)


def hops(offset):
    a, b = offset
    return steps(a // 4, 4) + steps(a % 4, 4) + steps(b // 2, 4) + 0.5 * (b % 2)


PARTNERS = sorted(((a, b) for a in range(GX) for b in range(GY) if a or b), key=hops, reverse=True)


def scope(name):
    return jax.named_scope(name) if SCOPES else contextlib.nullcontext()


def spectrum():
    k = np.arange(1, NZ + 1, dtype=np.float64)
    return 4.0 * np.sin(0.5 * np.pi * k / (NZ + 1)) ** 2


def sine_matrix(weight=1.0):
    k = np.arange(1, NZ + 1, dtype=np.float64)
    full = weight * (np.sqrt(2.0 / (NZ + 1)) * np.sin(np.pi * np.outer(k, k) / (NZ + 1)))
    return np.concatenate([full[0::2], full[1::2]]).astype(np.float32)


def eigenvalues():
    rows = np.tile(spectrum().reshape(NDEV, 2), (1, 4))
    return np.broadcast_to(rows[:, :, None], (NDEV, 8, 128)).astype(np.float32)


def iota(axis):
    return lax.broadcasted_iota(jnp.int32, (8, 128), axis)


def shifted_rows(a, edge, up):
    rows = a.shape[0]
    row = lax.broadcasted_iota(jnp.int32, a.shape, 0)
    if up:
        return jnp.where(row == rows - 1, edge, pltpu.roll(a, rows - 1, 0))
    return jnp.where(row == 0, edge, pltpu.roll(a, 1, 0))


def shifted_depth(a, up):
    depth = a.shape[1]
    col = lax.broadcasted_iota(jnp.int32, a.shape, 1)
    if up:
        return jnp.where(col == depth - 1, 0.0, pltpu.roll(a, depth - 1, 1))
    return jnp.where(col == 0, 0.0, pltpu.roll(a, 1, 1))


def transform(x, y, dim):
    return lax.dot_general(x, y, (((dim,), (dim,)), ((), ())), precision=HIGHEST, preferred_element_type=jnp.float32)


def split(x):
    high = x.astype(jnp.bfloat16)
    x = x - high.astype(jnp.float32)
    mid = x.astype(jnp.bfloat16)
    return high, mid, (x - mid.astype(jnp.float32)).astype(jnp.bfloat16)


def product(x, y):
    return lax.dot_general(x, y, (((1,), (0,)), ((), ())), preferred_element_type=jnp.float32)


def fence():
    pl.delay(1)


class Lanes:
    def __init__(self):
        gx = lax.rem(iota(1), GX)
        self.first, self.last = gx == 0, gx == GX - 1
        self.sub = iota(0)

    def from_left(self, v):
        return jnp.where(self.first, pltpu.roll(v, 128 - (GX - 1), 1), pltpu.roll(v, 1, 1))

    def from_right(self, v):
        return jnp.where(self.last, pltpu.roll(v, GX - 1, 1), pltpu.roll(v, 127, 1))

    def from_below(self, v):
        return pltpu.roll(v, GX, 1)

    def from_above(self, v):
        return pltpu.roll(v, 128 - GX, 1)


class Field:
    def __init__(self, level, ref=None):
        self.level, self.ref, self.held = level, ref, {}
        self.nx, self.ny = BX >> level, max(1, 4 >> level)
        self.step = max(1, (1 << level) // 4)

    def cells(self):
        return [(x, y) for x in range(self.nx) for y in range(self.ny)]

    def get(self, x, y):
        return self.held[x, y] if self.ref is None else self.ref[x, y]

    def put(self, x, y, value):
        if self.ref is None:
            self.held[x, y] = value
        else:
            self.ref[x, y] = value

    def beside(self, x, y, lanes):
        step = self.step
        left = self.get(x - 1, y) if x > 0 else lanes.from_left(self.get(self.nx - 1, y))
        right = self.get(x + 1, y) if x < self.nx - 1 else lanes.from_right(self.get(0, y))
        if y > 0:
            below = self.get(x, y - 1)
        else:
            below = pltpu.roll(self.get(x, self.ny - 1), step, 0)
            below = jnp.where(lanes.sub < step, lanes.from_below(below), below)
        if y < self.ny - 1:
            above = self.get(x, y + 1)
        else:
            above = pltpu.roll(self.get(x, 0), 8 - step, 0)
            above = jnp.where(lanes.sub >= 8 - step, lanes.from_above(above), above)
        return (left + right) + (below + above)


def weights(level):
    w = 0.25**level
    return w, OMEGA / (4.0 * w + 2.0)


def sweep(source, f, target, lam, lanes):
    w, c = weights(source.level)
    keep = 1.0 - c * (4.0 * w + lam)
    for x, y in source.cells():
        beside = source.beside(x, y, lanes)
        target.put(x, y, keep * source.get(x, y) + ((c * w) * beside + c * f.get(x, y)))


def first_two(f, target, lam, lanes):
    w, c = weights(f.level)
    keep = c * (2.0 - c * (4.0 * w + lam))
    for x, y in f.cells():
        target.put(x, y, keep * f.get(x, y) + (c * c * w) * f.beside(x, y, lanes))


def coarsen(source, f, coarse, lam, lanes):
    w, _ = weights(source.level)

    def rest(x, y):
        own = source.get(x, y)
        return f.get(x, y) - (w * (4.0 * own - source.beside(x, y, lanes)) + lam * own)

    for x, y in coarse.cells():
        if source.ny > 1:
            total = (rest(2 * x, 2 * y) + rest(2 * x + 1, 2 * y)) + (rest(2 * x, 2 * y + 1) + rest(2 * x + 1, 2 * y + 1))
        else:
            step = source.step
            both = rest(2 * x, y) + rest(2 * x + 1, y)
            even = lax.rem(lanes.sub // step, 2) == 0
            total = both + jnp.where(even, pltpu.roll(both, 8 - step, 0), pltpu.roll(both, step, 0))
        coarse.put(x, y, 0.25 * total)


def correct(target, e):
    for x, y in target.cells():
        target.put(x, y, target.get(x, y) + e.get(x // 2, y // 2 if target.ny > 1 else 0))


def coarsest(f, lam, lanes):
    level = f.level
    _, c = weights(level)
    own = f.get(0, 0)
    total = jnp.broadcast_to(jnp.sum(own, axis=1, keepdims=True), (8, 128))
    total = total + pltpu.roll(total, 4, 0)
    total = total + pltpu.roll(total, 2, 0)
    total = total + pltpu.roll(total, 1, 0)
    u = (total * (1.0 / 1024.0)) / lam
    decay = (1.0 - c * lam) * (1.0 - c * lam)
    v = Field(level)
    first_two(f, v, lam, lanes)
    for _ in range(2):
        new = Field(level)
        sweep(v, f, new, lam, lanes)
        v = new
    v.put(0, 0, v.get(0, 0) + (decay * decay) * u)
    return v


def kernel(
    f_hbm, p_hbm, s_hbm, st_hbm, lam_hbm,
    e_ref, r_ref, p_ref,
    f_ref, s_ref, st_ref, lam_ref, g_ref, o_ref, basis,
    send, recv, reply, back, w_ref, row_ref, f0, a0, b0, f1, a1, b1,
    in_sem, s_sem, r_sem,
):
    gx, gy = lax.axis_index("gx"), lax.axis_index("gy")
    me = gy * GX + gx
    loads = [
        pltpu.make_async_copy(source, target, in_sem.at[n])
        for n, (source, target) in enumerate(
            ((f_hbm, f_ref), (p_hbm, p_ref), (s_hbm, s_ref), (st_hbm, st_ref), (lam_hbm.at[me], lam_ref))
        )
    ]
    for load in loads:
        load.start()

    to_x = [lax.rem(gx + a, GX) for a in range(GX)]

    to_y = [lax.rem(gy + b, GY) for b in range(GY)]

    def partners(visit, order=PARTNERS):
        for a, b in order:
            visit(to_x[a], to_y[b])

    barrier = pltpu.get_barrier_semaphore()
    with scope("greet"):
        partners(lambda x, y: pl.semaphore_signal(barrier, inc=1, device_id=(x, y), device_id_type=MESH))
    with scope("load"):
        for load in loads:
            load.wait()

    with scope("stage_a"):
        g_ref[0:32] = f_ref[0, BX - 1] + p_ref[BX - 1]
        g_ref[32:64] = p_ref[0]
        g_ref[96:128] = jnp.zeros((32, NZ), jnp.float32)
        for i in range(BX):
            p, fx, fy, fz = p_ref[i], f_ref[0, i], f_ref[1, i], f_ref[2, i]
            r = shifted_depth(fz, False) - ((fx + fy + fz) + 4.0 * p)
            r = r + (shifted_rows(fy + p, 0.0, False) + shifted_rows(p, 0.0, True))
            if i > 0:
                r = r + (f_ref[0, i - 1] + p_ref[i - 1])
            if i < BX - 1:
                r = r + p_ref[i + 1]
            r_ref[i] = r
            g_ref[64 + i] = f_ref[1, i, BY - 1] + p_ref[i, BY - 1]
            g_ref[80 + i] = p_ref[i, 0]

    with scope("dst"):
        for t in range(4):
            rows = r_ref[4 * t : 4 * t + 4].reshape(128, NZ)
            flat = p_ref[4 * t : 4 * t + 4].reshape(128, NZ)
            o_ref[t] = transform(s_ref[...], rows, 1) + transform(st_ref[...], flat, 1)
        o_ref[4] = transform(s_ref[...], g_ref[...], 1)
    with scope("pack"):
        for k in range(2):
            for t in range(TILES):
                send[k, pl.ds(t, NDEV, stride=TILES), :] = o_ref[t, k * NDEV : (k + 1) * NDEV]

    with scope("basis"):
        for k in range(2):
            high, mid, low = split(s_ref[k * NDEV : (k + 1) * NDEV])
            for n, (first, second) in enumerate(((high, high), (mid, mid), (low, high))):
                basis[k, n, 0:NDEV] = first
                basis[k, n, NDEV : 2 * NDEV] = second

    with scope("barrier"):
        pl.semaphore_wait(barrier, NDEV - 1)

    def start_all_to_all(source, target, which, low=0, high=NDEV):
        mine = target.at[pl.ds(me * TILES, TILES)]

        def visit(x, y):
            pltpu.make_async_remote_copy(
                source.at[pl.ds((y * GX + x) * TILES, TILES)], mine, s_sem.at[which], r_sem.at[which],
                device_id=(x, y), device_id_type=MESH,
            ).start()

        partners(visit, PARTNERS[low:high])
        if low == 0:
            target[pl.ds(me * TILES, TILES), :] = source[pl.ds(me * TILES, TILES), :]

    def wait_all(ref, sem):
        most = ref.at[pl.ds(0, (NDEV - 1) * TILES)]
        pltpu.make_async_copy(most, most, sem).wait()

    with scope("a2a_1_start"):
        start_all_to_all(send.at[0], recv.at[0], 0)
        pl.delay(PAUSE)
        start_all_to_all(send.at[1], recv.at[1], 1)

    lanes = Lanes()

    def unpack(k):
        w = w_ref.at[k]
        for n in range(TILES):
            w[n] = recv[k, pl.ds(n, NDEV, stride=TILES), :].T
        for half in range(2):
            at = 8 * half
            row_ref[k, at : at + 8] = lanes.from_below(w[4, 64 + at : 72 + at])
            row_ref[k, 16 + at : 24 + at] = lanes.from_above(w[4, 80 + at : 88 + at])
        for x in range(BX):
            t, x4 = divmod(x, 4)
            for y in range(4):
                value = w[t, pl.ds(32 * x4 + y, 8, stride=4), :]
                if x == 0:
                    value = value + lanes.from_left(w[4, pl.ds(y, 8, stride=4), :])
                if x == BX - 1:
                    value = value + lanes.from_right(w[4, pl.ds(32 + y, 8, stride=4), :])
                if y == 0:
                    value = value + jnp.where(lanes.sub == 0, row_ref[k, x : x + 1], 0.0)
                if y == 3:
                    value = value + jnp.where(lanes.sub == 7, row_ref[k, 16 + x : 17 + x], 0.0)
                f0[k, x, y] = value

    lams = [jnp.broadcast_to(lam_ref[k : k + 1], (8, 128)) for k in range(2)]

    fields = [[(Field(0, f0.at[k]), Field(0, a0.at[k]), Field(0, b0.at[k])) for k in range(2)],
              [(Field(1, f1.at[k]), Field(1, a1.at[k]), Field(1, b1.at[k])) for k in range(2)]]

    def small(f, lam):
        level = f.level
        if level == LEVELS - 1:
            return coarsest(f, lam, lanes)
        v, coarse = Field(level), Field(level + 1)
        first_two(f, v, lam, lanes)
        coarsen(v, f, coarse, lam, lanes)
        correct(v, small(coarse, lam))
        for _ in range(2):
            new = Field(level)
            sweep(v, f, new, lam, lanes)
            v = new
        return v

    def cycle(k, level, first):
        f, a, b = fields[level][k]
        lam = lams[k]
        smooth = [
            (f"sweep_{level}", lambda: sweep(b, f, a, lam, lanes)),
            (f"sweep_{level}", lambda: sweep(a, f, b, lam, lanes)),
        ]
        passes = [(f"first_two_{level}", lambda: first_two(f, b, lam, lanes))] if first else list(smooth)
        if level == 0:
            passes.append(("coarsen_0", lambda: coarsen(b, f, fields[1][k][0], lam, lanes)))
            passes += cycle(k, 1, True)
            passes.append(("correct_0", lambda: correct(b, fields[1][k][2])))
        else:
            def inner():
                coarse = Field(2)
                coarsen(b, f, coarse, lam, lanes)
                correct(b, small(coarse, lam))

            passes.append((f"inner_{level}", inner))
        return passes + smooth

    def run(*lists):
        for together in zip(*lists, strict=True):
            with scope("+".join(name for name, _ in together)):
                for _, step in together:
                    step()
            fence()

    def gather_edges(k):
        w = w_ref.at[k]
        edge = w.at[4]
        for y in range(4):
            low = edge[pl.ds(y, 8, stride=4), :] + b0[k, BX - 1, y]
            high = edge[pl.ds(32 + y, 8, stride=4), :] + b0[k, 0, y]
            edge[pl.ds(y, 8, stride=4), :] = lanes.from_left(low)
            edge[pl.ds(32 + y, 8, stride=4), :] = lanes.from_right(high)
        for x in range(BX):
            edge[64 + x : 65 + x, :] = row_ref[k, x : x + 1] + lanes.from_below(b0[k, x, 3])[7:8]
            edge[80 + x : 81 + x, :] = row_ref[k, 16 + x : 17 + x] + lanes.from_above(b0[k, x, 0])[0:1]
            t, x4 = divmod(x, 4)
            for y in range(4):
                w[t, pl.ds(32 * x4 + y, 8, stride=4), :] = b0[k, x, y]

    def turn(k):
        for n in range(TILES):
            reply[k, pl.ds(n, NDEV, stride=TILES), :] = w_ref[k, n].T

    with scope("a2a_1_wait_0"):
        wait_all(recv.at[0], r_sem.at[0])
    run([("unpack", lambda: unpack(0))] + cycle(0, 0, True))
    run(cycle(0, 0, False) + [("gather", lambda: gather_edges(0)), ("turn", lambda: turn(0))])
    with scope("a2a_1_wait_1"):
        wait_all(recv.at[1], r_sem.at[1])
    early = [("unpack", lambda: unpack(1))] + cycle(1, 0, True)
    cuts = (0, 25, 42, 60, 72, NDEV - 1)
    sends = [
        ("send", functools.partial(start_all_to_all, reply.at[0], back.at[0], 2, low, high))
        for low, high in zip(cuts[:-1], cuts[1:])
    ]
    run(early[: len(sends)], sends)
    run(early[len(sends) :] + cycle(1, 0, False) + [("gather", lambda: gather_edges(1)), ("turn", lambda: turn(1))])
    with scope("a2a_2_start"):
        start_all_to_all(reply.at[1], back.at[1], 3)

    for k in range(2):
        with scope(f"a2a_2_wait_{k}"):
            wait_all(back.at[k], r_sem.at[2 + k])
        with scope("idst"):
            turned = jnp.concatenate([back[k, pl.ds(t, NDEV, stride=TILES), :].T for t in range(TILES)], axis=0)
            high, mid, low = split(turned)
            both, outer = jnp.concatenate([high, mid], axis=1), jnp.concatenate([high, low], axis=1)
            part = product(both, basis[k, 0]) + (product(both, basis[k, 1]) + product(outer, basis[k, 2]))
            e_ref[...] = part if k == 0 else e_ref[...] + part

    with scope("drain"):
        for k in range(2):
            wait_all(send.at[k], s_sem.at[k])
            wait_all(reply.at[k], s_sem.at[2 + k])


def finish(e_ref, r_ref, p_ref, pressure_hbm, residual_hbm, pressure_ref, residual_ref, sem):
    def plane(i):
        return e_ref[32 * i : 32 * i + 32]

    stores = []
    for i in range(BX):
        e = plane(i)
        p = p_ref[i] + e
        pressure_ref[i] = p
        r = r_ref[i] - 4.0 * e + (shifted_depth(p, False) + shifted_depth(p, True) - 2.0 * p)
        r = r + (shifted_rows(e, e_ref[576 + i : 577 + i], False) + shifted_rows(e, e_ref[592 + i : 593 + i], True))
        r = r + (plane(i - 1) if i > 0 else e_ref[512:544])
        r = r + (plane(i + 1) if i < BX - 1 else e_ref[544:576])
        residual_ref[i] = r
        if i % 4 == 3:
            part = pl.ds(i - 3, 4)
            for n, (source, target) in enumerate(((pressure_ref, pressure_hbm), (residual_ref, residual_hbm))):
                store = pltpu.make_async_copy(source.at[part], target.at[part], sem.at[n, i // 4])
                store.start()
                stores.append(store)
    for store in stores:
        store.wait()


def on_device(forces, pressure_prev):
    block = (BX, BY, NZ)
    anywhere = pl.BlockSpec(memory_space=pl.ANY)

    def vmem(*shape):
        return pltpu.VMEM(shape, jnp.float32)

    e, r, p = pl.pallas_call(
        kernel,
        out_shape=(vmem(TILES * 128, NZ), vmem(*block), vmem(*block)),
        in_specs=[anywhere] * 5,
        out_specs=(pl.BlockSpec(memory_space=pltpu.VMEM),) * 3,
        scratch_shapes=[
            vmem(3, *block), vmem(NZ, NZ), vmem(NZ, NZ), vmem(8, 128), vmem(128, NZ), vmem(TILES, NZ, 128), pltpu.VMEM((2, 3, NZ, NZ), jnp.bfloat16),
            *[vmem(2, NDEV * TILES, 128)] * 4, vmem(2, TILES, 128, 128), vmem(2, 32, 128),
            *[vmem(2, 16, 4, 8, 128)] * 3, *[vmem(2, 8, 2, 8, 128)] * 3,
            pltpu.SemaphoreType.DMA((5,)),
            pltpu.SemaphoreType.DMA((4,)),
            pltpu.SemaphoreType.DMA((4,)),
        ],
        compiler_params=pltpu.CompilerParams(collective_id=0, has_side_effects=True),
        name="poisson",
    )(
        forces,
        pressure_prev,
        jnp.asarray(sine_matrix()),
        jnp.asarray(sine_matrix(-spectrum()[:, None])),
        jnp.asarray(eigenvalues()),
    )
    e, r, p = (pltpu.with_memory_space_constraint(x, pltpu.VMEM) for x in (e, r, p))
    return pl.pallas_call(
        finish,
        out_shape=(jax.ShapeDtypeStruct(block, jnp.float32), jax.ShapeDtypeStruct(block, jnp.float32)),
        in_specs=[pl.BlockSpec(memory_space=pltpu.VMEM)] * 3,
        out_specs=(anywhere, anywhere),
        scratch_shapes=[vmem(*block), vmem(*block), pltpu.SemaphoreType.DMA((2, 4))],
        name="finish",
    )(e, r, p)


def solution(mesh):
    return jax.shard_map(
        on_device,
        mesh=mesh,
        in_specs=(P(None, "gx", "gy", None), P("gx", "gy", None)),
        out_specs=(P("gx", "gy", None), P("gx", "gy", None)),
        check_vma=False,
    )
```

```python
import contextlib
import functools

import jax
import jax.numpy as jnp
import numpy as np
from jax import lax
from jax.experimental import pallas as pl
from jax.experimental.pallas import tpu as pltpu
from jax.sharding import PartitionSpec as P

MESH = pl.DeviceIdType.MESH
OMEGA = 0.8
LEVELS = 5
GX, GY = 16, 8
NDEV = GX * GY
BX, BY, NZ = 16, 32, 256
TILES = 5
HIGHEST = lax.Precision.HIGHEST
SCOPES = False
PAUSE = 3600


def steps(distance, size):
    return min(distance, size - distance)


def hops(offset):
    a, b = offset
    return steps(a // 4, 4) + steps(a % 4, 4) + steps(b // 2, 4) + 0.5 * (b % 2)


PARTNERS = sorted(((a, b) for a in range(GX) for b in range(GY) if a or b), key=hops, reverse=True)


def scope(name):
    return jax.named_scope(name) if SCOPES else contextlib.nullcontext()


def spectrum():
    k = np.arange(1, NZ + 1, dtype=np.float64)
    return 4.0 * np.sin(0.5 * np.pi * k / (NZ + 1)) ** 2


def sine_matrix(weight=1.0):
    k = np.arange(1, NZ + 1, dtype=np.float64)
    full = weight * (np.sqrt(2.0 / (NZ + 1)) * np.sin(np.pi * np.outer(k, k) / (NZ + 1)))
    return np.concatenate([full[0::2], full[1::2]]).astype(np.float32)


def eigenvalues():
    rows = np.tile(spectrum().reshape(NDEV, 2), (1, 4))
    return np.broadcast_to(rows[:, :, None], (NDEV, 8, 128)).astype(np.float32)


def iota(axis):
    return lax.broadcasted_iota(jnp.int32, (8, 128), axis)


def shifted_rows(a, edge, up):
    rows = a.shape[0]
    row = lax.broadcasted_iota(jnp.int32, a.shape, 0)
    if up:
        return jnp.where(row == rows - 1, edge, pltpu.roll(a, rows - 1, 0))
    return jnp.where(row == 0, edge, pltpu.roll(a, 1, 0))


def shifted_depth(a, up):
    depth = a.shape[1]
    col = lax.broadcasted_iota(jnp.int32, a.shape, 1)
    if up:
        return jnp.where(col == depth - 1, 0.0, pltpu.roll(a, depth - 1, 1))
    return jnp.where(col == 0, 0.0, pltpu.roll(a, 1, 1))


def transform(x, y, dim):
    return lax.dot_general(x, y, (((dim,), (dim,)), ((), ())), precision=HIGHEST, preferred_element_type=jnp.float32)


def split(x):
    high = x.astype(jnp.bfloat16)
    x = x - high.astype(jnp.float32)
    mid = x.astype(jnp.bfloat16)
    return high, mid, (x - mid.astype(jnp.float32)).astype(jnp.bfloat16)


def product(x, y):
    return lax.dot_general(x, y, (((1,), (0,)), ((), ())), preferred_element_type=jnp.float32)


def fence():
    pl.delay(1)


class Lanes:
    def __init__(self):
        gx = lax.rem(iota(1), GX)
        self.first, self.last = gx == 0, gx == GX - 1
        self.sub = iota(0)

    def from_left(self, v):
        return jnp.where(self.first, pltpu.roll(v, 128 - (GX - 1), 1), pltpu.roll(v, 1, 1))

    def from_right(self, v):
        return jnp.where(self.last, pltpu.roll(v, GX - 1, 1), pltpu.roll(v, 127, 1))

    def from_below(self, v):
        return pltpu.roll(v, GX, 1)

    def from_above(self, v):
        return pltpu.roll(v, 128 - GX, 1)


class Field:
    def __init__(self, level, ref=None):
        self.level, self.ref, self.held = level, ref, {}
        self.nx, self.ny = BX >> level, max(1, 4 >> level)
        self.step = max(1, (1 << level) // 4)

    def cells(self):
        return [(x, y) for x in range(self.nx) for y in range(self.ny)]

    def get(self, x, y):
        return self.held[x, y] if self.ref is None else self.ref[x, y]

    def put(self, x, y, value):
        if self.ref is None:
            self.held[x, y] = value
        else:
            self.ref[x, y] = value

    def beside(self, x, y, lanes):
        step = self.step
        left = self.get(x - 1, y) if x > 0 else lanes.from_left(self.get(self.nx - 1, y))
        right = self.get(x + 1, y) if x < self.nx - 1 else lanes.from_right(self.get(0, y))
        if y > 0:
            below = self.get(x, y - 1)
        else:
            below = pltpu.roll(self.get(x, self.ny - 1), step, 0)
            below = jnp.where(lanes.sub < step, lanes.from_below(below), below)
        if y < self.ny - 1:
            above = self.get(x, y + 1)
        else:
            above = pltpu.roll(self.get(x, 0), 8 - step, 0)
            above = jnp.where(lanes.sub >= 8 - step, lanes.from_above(above), above)
        return (left + right) + (below + above)


def weights(level):
    w = 0.25**level
    return w, OMEGA / (4.0 * w + 2.0)


def sweep(source, f, target, lam, lanes):
    w, c = weights(source.level)
    keep = 1.0 - c * (4.0 * w + lam)
    for x, y in source.cells():
        beside = source.beside(x, y, lanes)
        target.put(x, y, keep * source.get(x, y) + ((c * w) * beside + c * f.get(x, y)))


def first_two(f, target, lam, lanes):
    w, c = weights(f.level)
    keep = c * (2.0 - c * (4.0 * w + lam))
    for x, y in f.cells():
        target.put(x, y, keep * f.get(x, y) + (c * c * w) * f.beside(x, y, lanes))


def coarsen(source, f, coarse, lam, lanes):
    w, _ = weights(source.level)

    def rest(x, y):
        own = source.get(x, y)
        return f.get(x, y) - (w * (4.0 * own - source.beside(x, y, lanes)) + lam * own)

    for x, y in coarse.cells():
        if source.ny > 1:
            total = (rest(2 * x, 2 * y) + rest(2 * x + 1, 2 * y)) + (rest(2 * x, 2 * y + 1) + rest(2 * x + 1, 2 * y + 1))
        else:
            step = source.step
            both = rest(2 * x, y) + rest(2 * x + 1, y)
            even = lax.rem(lanes.sub // step, 2) == 0
            total = both + jnp.where(even, pltpu.roll(both, 8 - step, 0), pltpu.roll(both, step, 0))
        coarse.put(x, y, 0.25 * total)


def correct(target, e):
    for x, y in target.cells():
        target.put(x, y, target.get(x, y) + e.get(x // 2, y // 2 if target.ny > 1 else 0))


def coarsest(f, lam, lanes):
    level = f.level
    _, c = weights(level)
    own = f.get(0, 0)
    total = jnp.broadcast_to(jnp.sum(own, axis=1, keepdims=True), (8, 128))
    total = total + pltpu.roll(total, 4, 0)
    total = total + pltpu.roll(total, 2, 0)
    total = total + pltpu.roll(total, 1, 0)
    u = (total * (1.0 / 1024.0)) / lam
    decay = (1.0 - c * lam) * (1.0 - c * lam)
    v = Field(level)
    first_two(f, v, lam, lanes)
    for _ in range(2):
        new = Field(level)
        sweep(v, f, new, lam, lanes)
        v = new
    v.put(0, 0, v.get(0, 0) + (decay * decay) * u)
    return v


def kernel(
    f_hbm, p_hbm, s_hbm, st_hbm, lam_hbm,
    e_ref, r_ref, p_ref,
    f_ref, s_ref, st_ref, lam_ref, g_ref, o_ref, basis,
    send, recv, reply, back, w_ref, row_ref, f0, a0, b0, f1, a1, b1,
    in_sem, s_sem, r_sem,
):
    gx, gy = lax.axis_index("gx"), lax.axis_index("gy")
    me = gy * GX + gx
    loads = [
        pltpu.make_async_copy(source, target, in_sem.at[n])
        for n, (source, target) in enumerate(
            ((f_hbm, f_ref), (p_hbm, p_ref), (s_hbm, s_ref), (st_hbm, st_ref), (lam_hbm.at[me], lam_ref))
        )
    ]
    for load in loads:
        load.start()

    to_x = [lax.rem(gx + a, GX) for a in range(GX)]

    to_y = [lax.rem(gy + b, GY) for b in range(GY)]

    def partners(visit, order=PARTNERS):
        for a, b in order:
            visit(to_x[a], to_y[b])

    barrier = pltpu.get_barrier_semaphore()
    with scope("greet"):
        partners(lambda x, y: pl.semaphore_signal(barrier, inc=1, device_id=(x, y), device_id_type=MESH))
    with scope("load"):
        for load in loads:
            load.wait()

    with scope("stage_a"):
        g_ref[0:32] = f_ref[0, BX - 1] + p_ref[BX - 1]
        g_ref[32:64] = p_ref[0]
        g_ref[96:128] = jnp.zeros((32, NZ), jnp.float32)
        for i in range(BX):
            p, fx, fy, fz = p_ref[i], f_ref[0, i], f_ref[1, i], f_ref[2, i]
            r = shifted_depth(fz, False) - ((fx + fy + fz) + 4.0 * p)
            r = r + (shifted_rows(fy + p, 0.0, False) + shifted_rows(p, 0.0, True))
            if i > 0:
                r = r + (f_ref[0, i - 1] + p_ref[i - 1])
            if i < BX - 1:
                r = r + p_ref[i + 1]
            r_ref[i] = r
            g_ref[64 + i] = f_ref[1, i, BY - 1] + p_ref[i, BY - 1]
            g_ref[80 + i] = p_ref[i, 0]

    with scope("dst"):
        for t in range(4):
            rows = r_ref[4 * t : 4 * t + 4].reshape(128, NZ)
            flat = p_ref[4 * t : 4 * t + 4].reshape(128, NZ)
            o_ref[t] = transform(s_ref[...], rows, 1) + transform(st_ref[...], flat, 1)
        o_ref[4] = transform(s_ref[...], g_ref[...], 1)
    with scope("pack"):
        for k in range(2):
            for t in range(TILES):
                send[k, pl.ds(t, NDEV, stride=TILES), :] = o_ref[t, k * NDEV : (k + 1) * NDEV]

    with scope("basis"):
        for k in range(2):
            high, mid, low = split(s_ref[k * NDEV : (k + 1) * NDEV])
            for n, (first, second) in enumerate(((high, high), (mid, mid), (low, high))):
                basis[k, n, 0:NDEV] = first
                basis[k, n, NDEV : 2 * NDEV] = second

    with scope("barrier"):
        pl.semaphore_wait(barrier, NDEV - 1)

    def start_all_to_all(source, target, which, low=0, high=NDEV):
        mine = target.at[pl.ds(me * TILES, TILES)]

        def visit(x, y):
            pltpu.make_async_remote_copy(
                source.at[pl.ds((y * GX + x) * TILES, TILES)], mine, s_sem.at[which], r_sem.at[which],
                device_id=(x, y), device_id_type=MESH,
            ).start()

        partners(visit, PARTNERS[low:high])
        if low == 0:
            target[pl.ds(me * TILES, TILES), :] = source[pl.ds(me * TILES, TILES), :]

    def wait_all(ref, sem):
        most = ref.at[pl.ds(0, (NDEV - 1) * TILES)]
        pltpu.make_async_copy(most, most, sem).wait()

    with scope("a2a_1_start"):
        start_all_to_all(send.at[0], recv.at[0], 0)
        pl.delay(PAUSE)
        start_all_to_all(send.at[1], recv.at[1], 1)

    lanes = Lanes()

    def unpack(k):
        w = w_ref.at[k]
        for n in range(TILES):
            w[n] = recv[k, pl.ds(n, NDEV, stride=TILES), :].T
        for half in range(2):
            at = 8 * half
            row_ref[k, at : at + 8] = lanes.from_below(w[4, 64 + at : 72 + at])
            row_ref[k, 16 + at : 24 + at] = lanes.from_above(w[4, 80 + at : 88 + at])
        for x in range(BX):
            t, x4 = divmod(x, 4)
            for y in range(4):
                value = w[t, pl.ds(32 * x4 + y, 8, stride=4), :]
                if x == 0:
                    value = value + lanes.from_left(w[4, pl.ds(y, 8, stride=4), :])
                if x == BX - 1:
                    value = value + lanes.from_right(w[4, pl.ds(32 + y, 8, stride=4), :])
                if y == 0:
                    value = value + jnp.where(lanes.sub == 0, row_ref[k, x : x + 1], 0.0)
                if y == 3:
                    value = value + jnp.where(lanes.sub == 7, row_ref[k, 16 + x : 17 + x], 0.0)
                f0[k, x, y] = value

    lams = [jnp.broadcast_to(lam_ref[k : k + 1], (8, 128)) for k in range(2)]

    fields = [[(Field(0, f0.at[k]), Field(0, a0.at[k]), Field(0, b0.at[k])) for k in range(2)],
              [(Field(1, f1.at[k]), Field(1, a1.at[k]), Field(1, b1.at[k])) for k in range(2)]]

    def small(f, lam):
        level = f.level
        if level == LEVELS - 1:
            return coarsest(f, lam, lanes)
        v, coarse = Field(level), Field(level + 1)
        first_two(f, v, lam, lanes)
        coarsen(v, f, coarse, lam, lanes)
        correct(v, small(coarse, lam))
        for _ in range(2):
            new = Field(level)
            sweep(v, f, new, lam, lanes)
            v = new
        return v

    def cycle(k, level, first):
        f, a, b = fields[level][k]
        lam = lams[k]
        smooth = [
            (f"sweep_{level}", lambda: sweep(b, f, a, lam, lanes)),
            (f"sweep_{level}", lambda: sweep(a, f, b, lam, lanes)),
        ]
        passes = [(f"first_two_{level}", lambda: first_two(f, b, lam, lanes))] if first else list(smooth)
        if level == 0:
            passes.append(("coarsen_0", lambda: coarsen(b, f, fields[1][k][0], lam, lanes)))
            passes += cycle(k, 1, True)
            passes.append(("correct_0", lambda: correct(b, fields[1][k][2])))
        else:
            def inner():
                coarse = Field(2)
                coarsen(b, f, coarse, lam, lanes)
                correct(b, small(coarse, lam))

            passes.append((f"inner_{level}", inner))
        return passes + smooth

    def run(*lists):
        for together in zip(*lists, strict=True):
            with scope("+".join(name for name, _ in together)):
                for _, step in together:
                    step()
            fence()

    def gather_edges(k):
        w = w_ref.at[k]
        edge = w.at[4]
        for y in range(4):
            low = edge[pl.ds(y, 8, stride=4), :] + b0[k, BX - 1, y]
            high = edge[pl.ds(32 + y, 8, stride=4), :] + b0[k, 0, y]
            edge[pl.ds(y, 8, stride=4), :] = lanes.from_left(low)
            edge[pl.ds(32 + y, 8, stride=4), :] = lanes.from_right(high)
        for x in range(BX):
            edge[64 + x : 65 + x, :] = row_ref[k, x : x + 1] + lanes.from_below(b0[k, x, 3])[7:8]
            edge[80 + x : 81 + x, :] = row_ref[k, 16 + x : 17 + x] + lanes.from_above(b0[k, x, 0])[0:1]
            t, x4 = divmod(x, 4)
            for y in range(4):
                w[t, pl.ds(32 * x4 + y, 8, stride=4), :] = b0[k, x, y]

    def turn(k):
        for n in range(TILES):
            reply[k, pl.ds(n, NDEV, stride=TILES), :] = w_ref[k, n].T

    with scope("a2a_1_wait_0"):
        wait_all(recv.at[0], r_sem.at[0])
    run([("unpack", lambda: unpack(0))] + cycle(0, 0, True))
    run(cycle(0, 0, False) + [("gather", lambda: gather_edges(0)), ("turn", lambda: turn(0))])
    with scope("a2a_1_wait_1"):
        wait_all(recv.at[1], r_sem.at[1])
    early = [("unpack", lambda: unpack(1))] + cycle(1, 0, True)
    cuts = (0, 25, 42, 60, 72, NDEV - 1)
    sends = [
        ("send", functools.partial(start_all_to_all, reply.at[0], back.at[0], 2, low, high))
        for low, high in zip(cuts[:-1], cuts[1:])
    ]
    run(early[: len(sends)], sends)
    run(early[len(sends) :] + cycle(1, 0, False) + [("gather", lambda: gather_edges(1))])
    with scope("turn+send"):
        turn(1)
        start_all_to_all(reply.at[1], back.at[1], 3)

    for k in range(2):
        with scope(f"a2a_2_wait_{k}"):
            wait_all(back.at[k], r_sem.at[2 + k])
        with scope("idst"):
            turned = jnp.concatenate([back[k, pl.ds(t, NDEV, stride=TILES), :].T for t in range(TILES)], axis=0)
            high, mid, low = split(turned)
            both, outer = jnp.concatenate([high, mid], axis=1), jnp.concatenate([high, low], axis=1)
            part = product(both, basis[k, 0]) + (product(both, basis[k, 1]) + product(outer, basis[k, 2]))
            e_ref[...] = part if k == 0 else e_ref[...] + part

    with scope("drain"):
        for k in range(2):
            wait_all(send.at[k], s_sem.at[k])
            wait_all(reply.at[k], s_sem.at[2 + k])


def finish(e_ref, r_ref, p_ref, pressure_hbm, residual_hbm, pressure_ref, residual_ref, sem):
    def plane(i):
        return e_ref[32 * i : 32 * i + 32]

    stores = []
    for i in range(BX):
        e = plane(i)
        p = p_ref[i] + e
        pressure_ref[i] = p
        r = r_ref[i] - 4.0 * e + (shifted_depth(p, False) + shifted_depth(p, True) - 2.0 * p)
        r = r + (shifted_rows(e, e_ref[576 + i : 577 + i], False) + shifted_rows(e, e_ref[592 + i : 593 + i], True))
        r = r + (plane(i - 1) if i > 0 else e_ref[512:544])
        r = r + (plane(i + 1) if i < BX - 1 else e_ref[544:576])
        residual_ref[i] = r
        if i % 2 == 1:
            part = pl.ds(i - 1, 2)
            for n, (source, target) in enumerate(((pressure_ref, pressure_hbm), (residual_ref, residual_hbm))):
                store = pltpu.make_async_copy(source.at[part], target.at[part], sem.at[n, i // 2])
                store.start()
                stores.append(store)
    for store in stores:
        store.wait()


def on_device(forces, pressure_prev):
    block = (BX, BY, NZ)
    anywhere = pl.BlockSpec(memory_space=pl.ANY)

    def vmem(*shape):
        return pltpu.VMEM(shape, jnp.float32)

    e, r, p = pl.pallas_call(
        kernel,
        out_shape=(vmem(TILES * 128, NZ), vmem(*block), vmem(*block)),
        in_specs=[anywhere] * 5,
        out_specs=(pl.BlockSpec(memory_space=pltpu.VMEM),) * 3,
        scratch_shapes=[
            vmem(3, *block), vmem(NZ, NZ), vmem(NZ, NZ), vmem(8, 128), vmem(128, NZ), vmem(TILES, NZ, 128), pltpu.VMEM((2, 3, NZ, NZ), jnp.bfloat16),
            *[vmem(2, NDEV * TILES, 128)] * 4, vmem(2, TILES, 128, 128), vmem(2, 32, 128),
            *[vmem(2, 16, 4, 8, 128)] * 3, *[vmem(2, 8, 2, 8, 128)] * 3,
            pltpu.SemaphoreType.DMA((5,)),
            pltpu.SemaphoreType.DMA((4,)),
            pltpu.SemaphoreType.DMA((4,)),
        ],
        compiler_params=pltpu.CompilerParams(collective_id=0, has_side_effects=True),
        name="poisson",
    )(
        forces,
        pressure_prev,
        jnp.asarray(sine_matrix()),
        jnp.asarray(sine_matrix(-spectrum()[:, None])),
        jnp.asarray(eigenvalues()),
    )
    e, r, p = (pltpu.with_memory_space_constraint(x, pltpu.VMEM) for x in (e, r, p))
    return pl.pallas_call(
        finish,
        out_shape=(jax.ShapeDtypeStruct(block, jnp.float32), jax.ShapeDtypeStruct(block, jnp.float32)),
        in_specs=[pl.BlockSpec(memory_space=pltpu.VMEM)] * 3,
        out_specs=(anywhere, anywhere),
        scratch_shapes=[vmem(*block), vmem(*block), pltpu.SemaphoreType.DMA((2, 8))],
        name="finish",
    )(e, r, p)


def solution(mesh):
    return jax.shard_map(
        on_device,
        mesh=mesh,
        in_specs=(P(None, "gx", "gy", None), P("gx", "gy", None)),
        out_specs=(P("gx", "gy", None), P("gx", "gy", None)),
        check_vma=False,
    )
```
